32 devices in a mesh: blk: 4 (over z), pts: 8 (over y, x, core).
Axes of the slice: x: 2, y: 2, z: 4, core: 2. Of those that a mesh axis runs over, the one named last changes fastest.
Arguments:
- signal: bfloat16 [67584, 2048], P('blk', 'pts'), may hold values from -6 to 6
- offsets: int32 [128], P('blk'), may hold values from 0 to 15872
- kept: int32 [16], replicated, may hold values from 0 to 512
- weights: float32 [2048], P('pts'), may hold values from 0.2 to 5
Outputs:
- gram: float32 [16, 2, 128, 128], P('pts', None, 'blk')
The draws below stay inside these ranges and needn't reach their ends.
Inputs may be any that keep to these rules, and one draw needn't show every extreme that they name: `kept`: indices may repeat.
All inputs are finite; a program needn't handle non-finite values.
Results may differ from the reference program's by a relative error of at most 0.0022.
Values may be sent and summed in bfloat16 or wider, within the bound.
A program may use at most 128 MiB of HBM per device.

```python
import math
import jax
import jax.numpy as jnp
from jax import lax

NFFT = 1024
BLK_DEV = 32
NB = 128
K = 16
POINTS = 2048
SEG = 16896
TIME = 67584


def place_ends(entries, own_key, low, top_value):
    shape = entries.shape
    place = [jax.random.randint(jax.random.fold_in(own_key, axis), (), 0, shape[axis]) for axis in range(len(shape))]
    entries = entries.at[tuple(place)].set(low)
    longest = shape.index(max(shape))
    place[longest] = (place[longest] + 1) % shape[longest]
    return entries.at[tuple(place)].set(top_value)


def block_scale(rng, shape, split, smallest, high):
    gain = 1.0
    for position, blocks in split:
        steps = jax.random.uniform(jax.random.fold_in(jax.random.fold_in(rng, 6), position), (blocks,), jnp.float32, smallest / len(split), high / len(split))
        gain = gain * jnp.repeat(jnp.exp(steps), shape[position] // blocks).reshape((-1,) + (1,) * (len(shape) - 1 - position))
    return gain


def normal_values(key, dims, scale, bound, split=(), kind=jnp.bfloat16):
    loudness = block_scale(key, dims, split, -0.22, 0.18) if split else 1.0
    entries = jax.random.normal(key, dims, jnp.float32) * scale * loudness
    return jnp.minimum(jnp.maximum(entries, -bound), bound).astype(kind)


def setup_inputs(seed: int = 0) -> dict:
    key_list = jax.random.split(jax.random.key(seed), 5)
    signal = normal_values(key_list[0], (TIME, POINTS), 1.0, 6.0, ((0, 4), (1, 8)))
    offsets = place_ends(jax.random.randint(key_list[1], (NB,), 0, SEG - NFFT + 1), jax.random.fold_in(key_list[1], 1), 0, SEG - NFFT).astype(jnp.int32)
    kept = place_ends(jax.random.randint(key_list[2], (K,), 0, NFFT // 2 + 1), jax.random.fold_in(key_list[2], 1), 0, (NFFT // 2 + 1) - 1).astype(jnp.int32)
    weights = jnp.clip(jnp.exp(math.log(5.0) - 3.218876 * jax.random.uniform(key_list[3], (POINTS,), jnp.float32) ** block_scale(key_list[3], (POINTS,), ((0, 8),), -0.2, 0.2)), 0.2, 5.0)
    return dict(signal=signal, offsets=offsets, kept=kept, weights=weights)


def spectral_table(kept, length):
    times = jnp.arange(length, dtype=jnp.int32)
    window = 0.5 - 0.5 * jnp.cos(times.astype(jnp.float32) * (2.0 * math.pi / length))
    norm = 1.0 / jnp.sqrt(jnp.sum(window * window))
    phase_index = times[:, None] * kept[None, :].astype(jnp.int32) % length
    phase = phase_index.astype(jnp.float32) * (2.0 * math.pi / length)
    cosine = (norm * window)[:, None] * jnp.cos(phase)
    sine = -(norm * window)[:, None] * jnp.sin(phase)
    return jnp.concatenate([cosine, sine], axis=1).astype(jnp.bfloat16)

def reference(signal, offsets, kept, weights):
    table = spectral_table(kept, NFFT).astype(jnp.float32)
    scale = jnp.sqrt(weights / POINTS)

    def one_block(index):
        start = index // BLK_DEV * SEG + offsets[index]
        block = lax.dynamic_slice(signal, (start.astype(jnp.int32), jnp.int32(0)), (NFFT, POINTS))
        values = jnp.dot(table.T, block.astype(jnp.float32), preferred_element_type=jnp.float32)
        return (values * scale[None, :]).astype(jnp.bfloat16).reshape(2, K, POINTS)
    spectra = lax.map(one_block, jnp.arange(NB, dtype=jnp.int32))

    def one_freq(index):
        part = lax.dynamic_index_in_dim(spectra, index, 2, keepdims=False)
        real_part = part[:, 0, :].astype(jnp.float32)
        imag_part = part[:, 1, :].astype(jnp.float32)
        gram_re = jnp.dot(real_part, real_part.T) + jnp.dot(imag_part, imag_part.T)
        gram_im = jnp.dot(real_part, imag_part.T) - jnp.dot(imag_part, real_part.T)
        return jnp.stack([gram_re, gram_im], axis=0)
    return lax.map(one_freq, jnp.arange(K, dtype=jnp.int32))
```

```python
import functools
import math

import jax
import jax.numpy as jnp
from jax import lax
from jax.experimental import pallas as pl
from jax.experimental.pallas import tpu as pltpu
from jax.sharding import PartitionSpec as P

NFFT = 1024
ALIGN = 16
LANES = 128
SPAN = NFFT + LANES
PIECES = 8
UNROLL = 8
MESH = pl.DeviceIdType.MESH


def fill_tables(kept_ref, table_ref):
    kept_all = kept_ref.shape[0]
    shape = (kept_all, NFFT)
    times = lax.broadcasted_iota(jnp.int32, shape, 1)
    row = lax.broadcasted_iota(jnp.int32, shape, 0)
    kept = jnp.zeros(shape, jnp.int32)
    for k in range(kept_all):
        kept = jnp.where(row == k, kept_ref[k], kept)
    step = 2.0 * math.pi / NFFT
    line = lax.broadcasted_iota(jnp.int32, (8, NFFT), 1)
    window = 0.5 - 0.5 * jnp.cos(line.astype(jnp.float32) * step)
    norm = 1.0 / jnp.sqrt(jnp.sum(window[:1] * window[:1], axis=1, keepdims=True))
    gain = norm * window[:1]
    phase = ((times * kept) & (NFFT - 1)).astype(jnp.float32) * step
    tail = jnp.zeros((2 * kept_all, SPAN - NFFT), jnp.float32)
    base = jnp.concatenate([gain * jnp.cos(phase), -gain * jnp.sin(phase)], axis=0)
    base = jnp.concatenate([base, tail], axis=1)
    for shift in range(ALIGN):
        moved = base if shift == 0 else pltpu.roll(base, shift, 1)
        table_ref[shift] = moved.astype(jnp.bfloat16)


def spectra_kernel(
    n_pts,
    signal_ref,
    offsets_ref,
    kept_ref,
    weights_ref,
    spec,
    held,
    table_ref,
    low,
    high,
    load_sem,
):
    seg, points = signal_ref.shape
    blocks = offsets_ref.shape[0]
    freq_all = kept_ref.shape[0]

    loads = []
    rows = seg // PIECES
    for piece in range(PIECES):
        copy = pltpu.make_async_copy(
            signal_ref.at[pl.ds(piece * rows, rows)],
            held.at[pl.ds(piece * rows, rows)],
            load_sem.at[piece],
        )
        copy.start()
        loads.append(copy)

    held[pl.ds(seg, LANES), :] = jnp.zeros((LANES, points), held.dtype)
    fill_tables(kept_ref, table_ref)
    for copy in loads:
        copy.wait()

    def some_blocks(turn, _):
        for inner in range(UNROLL):
            block = turn * UNROLL + inner
            start = offsets_ref[block]
            shift = start & (ALIGN - 1)
            rows_at = pl.multiple_of(start - shift, ALIGN)
            values = jnp.dot(
                table_ref[shift],
                held[pl.ds(rows_at, SPAN), :],
                preferred_element_type=jnp.float32,
            )
            low[pl.ds(block, 2 * freq_all, stride=blocks), :] = values[:, :LANES]
            high[pl.ds(block, 2 * freq_all, stride=blocks), :] = values[:, LANES:]
        return 0

    lax.fori_loop(0, blocks // UNROLL, some_blocks, 0)

    scale = jnp.sqrt(weights_ref[...] / (points * n_pts))

    for c in range(2):
        for k in range(freq_all):
            at = pl.ds((c * freq_all + k) * blocks, blocks)
            both = jnp.concatenate([low[at, :], high[at, :]], axis=1)
            spec[c, k] = (both * scale).astype(jnp.bfloat16)


def gram_kernel(
    n_blk,
    n_pts,
    spec,
    out_ref,
    got,
    gram,
    part,
    far,
    send_sem,
    recv_sem,
    send2_sem,
    recv2_sem,
):
    freq_all, blocks, points = spec.shape[1:]
    freqs = freq_all // n_pts
    groups = n_pts // n_blk
    mine = lax.axis_index("blk")
    col = lax.axis_index("pts")

    def target(step):
        dest = lax.rem(col + step, n_pts)
        return lax.rem(col + dest, n_blk), dest

    def source(group, step):
        origin = lax.rem(mine + n_blk - lax.rem(col, n_blk), n_blk) + group * n_blk
        return lax.rem(mine + step, n_blk), origin

    barrier = pltpu.get_barrier_semaphore()

    def greet(where):
        pl.semaphore_signal(barrier, inc=1, device_id=where, device_id_type=MESH)

    for step in range(n_pts):
        greet(target(step))
    for group in range(groups):
        for step in range(n_blk):
            greet(source(group, step))
    for step in range(1, n_blk):
        where = (lax.rem(mine + step, n_blk), col)
        pl.semaphore_signal(barrier, inc=1, device_id=where, device_id_type=MESH)

    pl.semaphore_wait(barrier, 2 * n_pts + n_blk - 1)

    slot = lax.div(col, n_blk)

    def send(step):
        where = target(step)
        return pltpu.make_async_remote_copy(
            src_ref=spec.at[:, pl.ds(where[1] * freqs, freqs)],
            dst_ref=got.at[slot, :, :, mine],
            send_sem=send_sem.at[step],
            recv_sem=recv_sem.at[slot, mine],
            device_id=where,
            device_id_type=MESH,
        )

    own = lax.rem(2 * col, n_blk) == mine

    @pl.when(own)
    def _():
        pltpu.make_async_copy(
            spec.at[:, pl.ds(col * freqs, freqs)],
            got.at[slot, :, :, mine],
            recv_sem.at[slot, mine],
        ).start()

    @pl.when(jnp.logical_not(own))
    def _():
        send(0).start()

    for step in range(1, n_pts):
        send(step).start()

    for group in range(groups):
        for z in range(n_blk):
            pltpu.make_async_copy(
                spec.at[:, pl.ds(0, freqs)], got.at[group, :, :, z], recv_sem.at[group, z]
            ).wait()

    whole = n_blk * blocks
    for f in range(freqs):
        total = jnp.zeros((2 * whole, 2 * whole), jnp.float32)
        for group in range(groups):
            x = jnp.concatenate(
                [
                    got[group, 0, f].reshape(whole, points),
                    got[group, 1, f].reshape(whole, points),
                ],
                axis=0,
            )
            total = total + lax.dot_general(
                x, x, (((1,), (1,)), ((), ())), preferred_element_type=jnp.float32
            )
        real = total[:whole, :whole] + total[whole:, whole:]
        imag = total[:whole, whole:] - total[whole:, :whole]
        for c, value in ((0, real), (1, imag)):
            for z in range(n_blk):
                rows_z = value[z * blocks : (z + 1) * blocks]
                gram[z, f, c] = rows_z
                part[z, f, c] = rows_z.astype(jnp.bfloat16)

    def give(step):
        to = lax.rem(mine + step, n_blk)
        return pltpu.make_async_remote_copy(
            src_ref=part.at[to],
            dst_ref=far.at[step - 1],
            send_sem=send2_sem.at[step - 1],
            recv_sem=recv2_sem.at[step - 1],
            device_id=(to, col),
            device_id_type=MESH,
        )

    for step in range(1, n_blk):
        give(step).start()
    result = gram[mine]
    for step in range(1, n_blk):
        give(step).wait_recv()
        result = result + far[step - 1].astype(jnp.float32)
    out_ref[...] = result

    for step in range(1, n_blk):
        give(step).wait_send()

    @pl.when(jnp.logical_not(own))
    def _():
        send(0).wait_send()

    for step in range(1, n_pts):
        send(step).wait_send()


def on_device(n_blk, n_pts, signal, offsets, kept, weights):
    seg, points = signal.shape
    blocks = offsets.shape[0]
    freq_all = kept.shape[0]
    freqs = freq_all // n_pts
    groups = n_pts // n_blk
    whole = n_blk * blocks
    vmem = pl.BlockSpec(memory_space=pltpu.VMEM)
    smem = pl.BlockSpec(memory_space=pltpu.SMEM)
    spec = pl.pallas_call(
        functools.partial(spectra_kernel, n_pts),
        out_shape=jax.ShapeDtypeStruct((2, freq_all, blocks, points), jnp.bfloat16),
        in_specs=[pl.BlockSpec(memory_space=pl.ANY), smem, smem, vmem],
        out_specs=vmem,
        scratch_shapes=[
            pltpu.VMEM((seg + LANES, points), jnp.bfloat16),
            pltpu.VMEM((ALIGN, 2 * freq_all, SPAN), jnp.bfloat16),
            pltpu.VMEM((2 * freq_all * blocks, LANES), jnp.float32),
            pltpu.VMEM((2 * freq_all * blocks, LANES), jnp.float32),
            pltpu.SemaphoreType.DMA((PIECES,)),
        ],
        compiler_params=pltpu.CompilerParams(vmem_limit_bytes=48 * 1024 * 1024),
    )(signal, offsets, kept, weights.reshape(1, points))
    return pl.pallas_call(
        functools.partial(gram_kernel, n_blk, n_pts),
        out_shape=jax.ShapeDtypeStruct((freqs, 2, blocks, whole), jnp.float32),
        in_specs=[vmem],
        out_specs=vmem,
        scratch_shapes=[
            pltpu.VMEM((groups, 2, freqs, n_blk, blocks, points), jnp.bfloat16),
            pltpu.VMEM((n_blk, freqs, 2, blocks, whole), jnp.float32),
            pltpu.VMEM((n_blk, freqs, 2, blocks, whole), jnp.bfloat16),
            pltpu.VMEM((n_blk - 1, freqs, 2, blocks, whole), jnp.bfloat16),
            pltpu.SemaphoreType.DMA((n_pts,)),
            pltpu.SemaphoreType.DMA((groups, n_blk)),
            pltpu.SemaphoreType.DMA((n_blk - 1,)),
            pltpu.SemaphoreType.DMA((n_blk - 1,)),
        ],
        compiler_params=pltpu.CompilerParams(
            collective_id=0, has_side_effects=True, vmem_limit_bytes=32 * 1024 * 1024
        ),
    )(spec)


def solution(mesh):
    placed = (P("blk", "pts"), P("blk"), P(), P("pts"))
    return jax.shard_map(
        functools.partial(on_device, mesh.shape["blk"], mesh.shape["pts"]),
        mesh=mesh,
        in_specs=placed,
        out_specs=P("pts", None, "blk", None),
        check_vma=False,
    )
```

```python
import functools
import math

import jax
import jax.numpy as jnp
from jax import lax
from jax.experimental import pallas as pl
from jax.experimental.pallas import tpu as pltpu
from jax.sharding import PartitionSpec as P

NFFT = 1024
ALIGN = 16
LANES = 128
SPAN = NFFT + LANES
PIECES = 8
UNROLL = 8
STAGES = 2
MESH = pl.DeviceIdType.MESH


def fill_tables(kept_ref, table_ref):
    kept_all = kept_ref.shape[0]
    shape = (kept_all, NFFT)
    times = lax.broadcasted_iota(jnp.int32, shape, 1)
    row = lax.broadcasted_iota(jnp.int32, shape, 0)
    kept = jnp.zeros(shape, jnp.int32)
    for k in range(kept_all):
        kept = jnp.where(row == k, kept_ref[k], kept)
    step = 2.0 * math.pi / NFFT
    line = lax.broadcasted_iota(jnp.int32, (8, NFFT), 1)
    window = 0.5 - 0.5 * jnp.cos(line.astype(jnp.float32) * step)
    norm = 1.0 / jnp.sqrt(jnp.sum(window[:1] * window[:1], axis=1, keepdims=True))
    gain = norm * window[:1]
    phase = ((times * kept) & (NFFT - 1)).astype(jnp.float32) * step
    tail = jnp.zeros((2 * kept_all, SPAN - NFFT), jnp.float32)
    base = jnp.concatenate([gain * jnp.cos(phase), -gain * jnp.sin(phase)], axis=0)
    base = jnp.concatenate([base, tail], axis=1)
    for shift in range(ALIGN):
        moved = base if shift == 0 else pltpu.roll(base, shift, 1)
        table_ref[shift] = moved.astype(jnp.bfloat16)


def kernel(
    n_blk,
    n_pts,
    signal_ref,
    offsets_hbm,
    kept_hbm,
    weights_hbm,
    out_ref,
    held,
    table_ref,
    low,
    high,
    spec,
    got,
    gram,
    part,
    far,
    offsets_ref,
    kept_ref,
    weights_ref,
    load_sem,
    send_sem,
    recv_sem,
    send2_sem,
    recv2_sem,
):
    tiles, _, points = signal_ref.shape
    blocks = offsets_ref.shape[0]
    freq_all = kept_ref.shape[0]
    freqs = freq_all // n_pts
    groups = n_pts // n_blk
    stage_blocks = blocks // STAGES
    mine = lax.axis_index("blk")
    col = lax.axis_index("pts")

    smalls = [
        pltpu.make_async_copy(kept_hbm, kept_ref, load_sem.at[PIECES]),
        pltpu.make_async_copy(offsets_hbm, offsets_ref, load_sem.at[PIECES + 1]),
        pltpu.make_async_copy(weights_hbm, weights_ref, load_sem.at[PIECES + 2]),
    ]
    loads = []
    rows = tiles // PIECES
    for piece in range(PIECES):
        at = pl.ds(piece * rows, rows)
        loads.append(
            pltpu.make_async_copy(signal_ref.at[at], held.at[at], load_sem.at[piece])
        )
    for copy in smalls + loads:
        copy.start()

    def target(step):
        dest = lax.rem(col + step, n_pts)
        return lax.rem(col + dest, n_blk), dest

    def source(group, step):
        origin = lax.rem(mine + n_blk - lax.rem(col, n_blk), n_blk) + group * n_blk
        return lax.rem(mine + step, n_blk), origin

    barrier = pltpu.get_barrier_semaphore()

    def greet(where):
        pl.semaphore_signal(barrier, inc=1, device_id=where, device_id_type=MESH)

    for step in range(n_pts):
        greet(target(step))
    for group in range(groups):
        for step in range(n_blk):
            greet(source(group, step))
    for step in range(1, n_blk):
        greet((lax.rem(mine + step, n_blk), col))

    held[pl.ds(tiles, LANES // ALIGN)] = jnp.zeros(
        (LANES // ALIGN, ALIGN, points), held.dtype
    )
    for copy in smalls:
        copy.wait()
    fill_tables(kept_ref, table_ref)
    scale = jnp.sqrt(weights_ref[...] / (points * n_pts))
    for copy in loads:
        copy.wait()

    slot = lax.div(col, n_blk)
    own = lax.rem(2 * col, n_blk) == mine

    def landing(stage):
        return got.at[slot, :, :, mine, pl.ds(stage * stage_blocks, stage_blocks)]

    def send(stage, step):
        where = target(step)
        return pltpu.make_async_remote_copy(
            src_ref=spec.at[stage, :, pl.ds(where[1] * freqs, freqs)],
            dst_ref=landing(stage),
            send_sem=send_sem.at[stage, step],
            recv_sem=recv_sem.at[stage, slot, mine],
            device_id=where,
            device_id_type=MESH,
        )

    for stage in range(STAGES):

        def some_blocks(turn, _):
            for inner in range(UNROLL):
                block = turn * UNROLL + inner
                start = offsets_ref[stage * stage_blocks + block]
                shift = start & (ALIGN - 1)
                tile = lax.div(start - shift, ALIGN)
                piece = jnp.concatenate(
                    [held[tile + part_at] for part_at in range(SPAN // ALIGN)], axis=0
                )
                values = jnp.dot(
                    table_ref[shift],
                    piece,
                    preferred_element_type=jnp.float32,
                )
                at = pl.ds(block, 2 * freq_all, stride=stage_blocks)
                low[stage, at, :] = values[:, :LANES]
                high[stage, at, :] = values[:, LANES:]
            return 0

        lax.fori_loop(0, stage_blocks // UNROLL, some_blocks, 0)

        for c in range(2):
            for k in range(freq_all):
                at = pl.ds((c * freq_all + k) * stage_blocks, stage_blocks)
                both = jnp.concatenate([low[stage, at, :], high[stage, at, :]], axis=1)
                spec[stage, c, k] = (both * scale).astype(jnp.bfloat16)

        if stage == 0:
            pl.semaphore_wait(barrier, 2 * n_pts + n_blk - 1)

        for step in range(1, n_pts):
            send(stage, step).start()

        @pl.when(jnp.logical_not(own))
        def _():
            send(stage, 0).start()

        @pl.when(own)
        def _():
            pltpu.make_async_copy(
                spec.at[stage, :, pl.ds(col * freqs, freqs)],
                landing(stage),
                recv_sem.at[stage, slot, mine],
            ).start()

    for stage in range(STAGES):
        for group in range(groups):
            for z in range(n_blk):
                pltpu.make_async_copy(
                    spec.at[stage, :, pl.ds(0, freqs)],
                    got.at[
                        group, :, :, z, pl.ds(stage * stage_blocks, stage_blocks)
                    ],
                    recv_sem.at[stage, group, z],
                ).wait()

    whole = n_blk * blocks
    for f in range(freqs):
        total = jnp.zeros((2 * whole, 2 * whole), jnp.float32)
        for group in range(groups):
            x = jnp.concatenate(
                [
                    got[group, 0, f].reshape(whole, points),
                    got[group, 1, f].reshape(whole, points),
                ],
                axis=0,
            )
            total = total + lax.dot_general(
                x, x, (((1,), (1,)), ((), ())), preferred_element_type=jnp.float32
            )
        real = total[:whole, :whole] + total[whole:, whole:]
        imag = total[:whole, whole:] - total[whole:, :whole]
        for c, value in ((0, real), (1, imag)):
            for z in range(n_blk):
                rows_z = value[z * blocks : (z + 1) * blocks]
                gram[z, f, c] = rows_z
                part[z, f, c] = rows_z.astype(jnp.bfloat16)

    def give(step):
        to = lax.rem(mine + step, n_blk)
        return pltpu.make_async_remote_copy(
            src_ref=part.at[to],
            dst_ref=far.at[step - 1],
            send_sem=send2_sem.at[step - 1],
            recv_sem=recv2_sem.at[step - 1],
            device_id=(to, col),
            device_id_type=MESH,
        )

    for step in range(1, n_blk):
        give(step).start()
    result = gram[mine]
    for step in range(1, n_blk):
        give(step).wait_recv()
        result = result + far[step - 1].astype(jnp.float32)
    out_ref[...] = result

    for step in range(1, n_blk):
        give(step).wait_send()

    for stage in range(STAGES):
        for step in range(1, n_pts):
            send(stage, step).wait_send()

        @pl.when(jnp.logical_not(own))
        def _():
            send(stage, 0).wait_send()


def on_device(n_blk, n_pts, signal, offsets, kept, weights):
    seg, points = signal.shape
    blocks = offsets.shape[0]
    freq_all = kept.shape[0]
    freqs = freq_all // n_pts
    groups = n_pts // n_blk
    whole = n_blk * blocks
    hbm = pl.BlockSpec(memory_space=pltpu.HBM)
    return pl.pallas_call(
        functools.partial(kernel, n_blk, n_pts),
        out_shape=jax.ShapeDtypeStruct((freqs, 2, blocks, whole), jnp.float32),
        in_specs=[hbm, hbm, hbm, hbm],
        out_specs=pl.BlockSpec(memory_space=pltpu.VMEM),
        scratch_shapes=[
            pltpu.VMEM(((seg + LANES) // ALIGN, ALIGN, points), jnp.bfloat16),
            pltpu.VMEM((ALIGN, 2 * freq_all, SPAN), jnp.bfloat16),
            pltpu.VMEM((STAGES, 2 * freq_all * blocks // STAGES, LANES), jnp.float32),
            pltpu.VMEM((STAGES, 2 * freq_all * blocks // STAGES, LANES), jnp.float32),
            pltpu.VMEM((STAGES, 2, freq_all, blocks // STAGES, points), jnp.bfloat16),
            pltpu.VMEM((groups, 2, freqs, n_blk, blocks, points), jnp.bfloat16),
            pltpu.VMEM((n_blk, freqs, 2, blocks, whole), jnp.float32),
            pltpu.VMEM((n_blk, freqs, 2, blocks, whole), jnp.bfloat16),
            pltpu.VMEM((n_blk - 1, freqs, 2, blocks, whole), jnp.bfloat16),
            pltpu.SMEM(offsets.shape, jnp.int32),
            pltpu.SMEM(kept.shape, jnp.int32),
            pltpu.VMEM((1, points), jnp.float32),
            pltpu.SemaphoreType.DMA((PIECES + 3,)),
            pltpu.SemaphoreType.DMA((STAGES, n_pts)),
            pltpu.SemaphoreType.DMA((STAGES, groups, n_blk)),
            pltpu.SemaphoreType.DMA((n_blk - 1,)),
            pltpu.SemaphoreType.DMA((n_blk - 1,)),
        ],
        compiler_params=pltpu.CompilerParams(
            collective_id=0, has_side_effects=True, vmem_limit_bytes=60000 * 1024
        ),
    )(
        signal.reshape(seg // ALIGN, ALIGN, points),
        offsets,
        kept,
        weights.reshape(1, points),
    )


def solution(mesh):
    placed = (P("blk", "pts"), P("blk"), P(), P("pts"))
    return jax.shard_map(
        functools.partial(on_device, mesh.shape["blk"], mesh.shape["pts"]),
        mesh=mesh,
        in_specs=placed,
        out_specs=P("pts", None, "blk", None),
        check_vma=False,
    )
```

```python
import functools
import math

import jax
import jax.numpy as jnp
from jax import lax
from jax.experimental import pallas as pl
from jax.experimental.pallas import tpu as pltpu
from jax.sharding import PartitionSpec as P

NFFT = 1024
ALIGN = 16
LANES = 128
SPAN = NFFT + LANES
PIECES = 4
UNROLL = 8
STAGES = 2
MESH = pl.DeviceIdType.MESH


def fill_tables(kept_ref, table_ref):
    kept_all = kept_ref.shape[0]
    shape = (kept_all, NFFT)
    times = lax.broadcasted_iota(jnp.int32, shape, 1)
    row = lax.broadcasted_iota(jnp.int32, shape, 0)
    kept = jnp.zeros(shape, jnp.int32)
    for k in range(kept_all):
        kept = jnp.where(row == k, kept_ref[k], kept)
    step = 2.0 * math.pi / NFFT
    line = lax.broadcasted_iota(jnp.int32, (8, NFFT), 1)
    window = 0.5 - 0.5 * jnp.cos(line.astype(jnp.float32) * step)
    norm = 1.0 / jnp.sqrt(jnp.sum(window[:1] * window[:1], axis=1, keepdims=True))
    gain = norm * window[:1]
    phase = ((times * kept) & (NFFT - 1)).astype(jnp.float32) * step
    tail = jnp.zeros((2 * kept_all, SPAN - NFFT), jnp.float32)
    base = jnp.concatenate([gain * jnp.cos(phase), -gain * jnp.sin(phase)], axis=0)
    base = jnp.concatenate([base, tail], axis=1)
    for shift in range(ALIGN):
        moved = base if shift == 0 else pltpu.roll(base, shift, 1)
        table_ref[shift] = moved.astype(jnp.bfloat16)


def kernel(
    n_blk,
    n_pts,
    signal_ref,
    offsets_hbm,
    kept_hbm,
    weights_hbm,
    out_ref,
    held,
    table_ref,
    sums,
    spec,
    got,
    square,
    gram,
    part,
    far,
    offsets_ref,
    kept_ref,
    weights_ref,
    load_sem,
    small_sem,
    send_sem,
    recv_sem,
    send2_sem,
    recv2_sem,
):
    tiles, _, points = signal_ref.shape
    blocks = offsets_ref.shape[0]
    freq_all = kept_ref.shape[0]
    freqs = freq_all // n_pts
    groups = n_pts // n_blk
    stage_blocks = blocks // STAGES
    halves = points // LANES
    mine = lax.axis_index("blk")
    col = lax.axis_index("pts")

    smalls = [
        pltpu.make_async_copy(kept_hbm, kept_ref, small_sem.at[0]),
        pltpu.make_async_copy(offsets_hbm, offsets_ref, small_sem.at[1]),
        pltpu.make_async_copy(weights_hbm, weights_ref, small_sem.at[2]),
    ]
    loads = []
    rows = tiles // PIECES
    for half in range(halves):
        lanes = pl.ds(half * LANES, LANES)
        for piece in range(PIECES):
            at = pl.ds(piece * rows, rows)
            loads.append(
                pltpu.make_async_copy(
                    signal_ref.at[at, :, lanes], held[half].at[at], load_sem.at[half, piece]
                )
            )
    for copy in smalls + loads:
        copy.start()

    slot = lax.div(col, n_blk)
    near = n_blk // 2
    first = lax.rem(lax.div(mine, near) * near + near, n_blk)

    def target(step):
        turn, group = step // groups, step % groups
        quarter = lax.rem(first + turn, n_blk)
        dest = lax.rem(quarter + n_blk - lax.rem(col, n_blk), n_blk)
        return quarter, dest + n_blk * lax.rem(slot + group, groups)

    def source(group, step):
        origin = lax.rem(mine + n_blk - lax.rem(col, n_blk), n_blk) + group * n_blk
        return lax.rem(mine + step, n_blk), origin

    barrier = pltpu.get_barrier_semaphore()

    def greet(where):
        pl.semaphore_signal(barrier, inc=1, device_id=where, device_id_type=MESH)

    for step in range(n_pts):
        greet(target(step))
    for group in range(groups):
        for step in range(n_blk):
            greet(source(group, step))
    for step in range(1, n_blk):
        greet((lax.rem(mine + step, n_blk), col))

    for half in range(halves):
        held[half][pl.ds(tiles, LANES // ALIGN)] = jnp.zeros(
            (LANES // ALIGN, ALIGN, LANES), jnp.bfloat16
        )
    for copy in smalls:
        copy.wait()
    fill_tables(kept_ref, table_ref)
    scale = jnp.sqrt(weights_ref[...] / (points * n_pts))

    def landing(half, stage):
        at = pl.ds(stage * stage_blocks, stage_blocks)
        return got.at[half, slot, :, :, mine, at]

    def send(half, stage, step):
        where = target(step)
        return pltpu.make_async_remote_copy(
            src_ref=spec.at[half, stage, :, pl.ds(where[1] * freqs, freqs)],
            dst_ref=landing(half, stage),
            send_sem=send_sem.at[half, stage, step],
            recv_sem=recv_sem.at[half, stage, slot, mine],
            device_id=where,
            device_id_type=MESH,
        )

    def unless_here(step, act):
        if step < near * groups:
            act()
        else:
            where = target(step)
            here = (where[0] == mine) & (where[1] == col)
            pl.when(jnp.logical_not(here))(act)

    own = lax.rem(2 * col, n_blk) == mine

    for half in range(halves):
        for copy in loads[half * PIECES : (half + 1) * PIECES]:
            copy.wait()
        for stage in range(STAGES):

            def some_blocks(turn, _):
                for inner in range(UNROLL):
                    block = turn * UNROLL + inner
                    start = offsets_ref[stage * stage_blocks + block]
                    shift = start & (ALIGN - 1)
                    tile = lax.div(start - shift, ALIGN)
                    piece = jnp.concatenate(
                        [held[half][tile + i] for i in range(SPAN // ALIGN)], axis=0
                    )
                    at = pl.ds(block, 2 * freq_all, stride=stage_blocks)
                    sums[half, stage, at, :] = jnp.dot(
                        table_ref[shift], piece, preferred_element_type=jnp.float32
                    )
                return 0

            lax.fori_loop(0, stage_blocks // UNROLL, some_blocks, 0)

            gains = scale[:, half * LANES : (half + 1) * LANES]
            for c in range(2):
                for k in range(freq_all):
                    at = pl.ds((c * freq_all + k) * stage_blocks, stage_blocks)
                    value = sums[half, stage, at, :] * gains
                    spec[half, stage, c, k] = value.astype(jnp.bfloat16)

            if half == 0 and stage == 0:
                pl.semaphore_wait(barrier, 2 * n_pts + n_blk - 1)

            for step in range(n_pts):
                unless_here(step, lambda: send(half, stage, step).start())

            @pl.when(own)
            def _():
                pltpu.make_async_copy(
                    spec.at[half, stage, :, pl.ds(col * freqs, freqs)],
                    landing(half, stage),
                    recv_sem.at[half, stage, slot, mine],
                ).start()

    whole = n_blk * blocks
    for half in range(halves):
        for stage in range(STAGES):
            at = pl.ds(stage * stage_blocks, stage_blocks)
            for group in range(groups):
                for z in range(n_blk):
                    pltpu.make_async_copy(
                        spec.at[half, stage, :, pl.ds(0, freqs)],
                        got.at[half, group, :, :, z, at],
                        recv_sem.at[half, stage, group, z],
                    ).wait()
        for f in range(freqs):
            x = jnp.concatenate(
                [
                    got[half, group, :, f].reshape(2 * whole, LANES)
                    for group in range(groups)
                ],
                axis=1,
            )
            term = lax.dot_general(
                x, x, (((1,), (1,)), ((), ())), preferred_element_type=jnp.float32
            )
            square[f] = term if half == 0 else square[f] + term

    for f in range(freqs):
        total = square[f]
        real = total[:whole, :whole] + total[whole:, whole:]
        imag = total[:whole, whole:] - total[whole:, :whole]
        for c, value in ((0, real), (1, imag)):
            for z in range(n_blk):
                rows_z = value[z * blocks : (z + 1) * blocks]
                gram[z, f, c] = rows_z
                part[z, f, c] = rows_z.astype(jnp.bfloat16)

    def give(step):
        to = lax.rem(mine + step, n_blk)
        return pltpu.make_async_remote_copy(
            src_ref=part.at[to],
            dst_ref=far.at[step - 1],
            send_sem=send2_sem.at[step - 1],
            recv_sem=recv2_sem.at[step - 1],
            device_id=(to, col),
            device_id_type=MESH,
        )

    for step in range(1, n_blk):
        give(step).start()
    result = gram[mine]
    for step in range(1, n_blk):
        give(step).wait_recv()
        result = result + far[step - 1].astype(jnp.float32)
    out_ref[...] = result

    for step in range(1, n_blk):
        give(step).wait_send()

    for half in range(halves):
        for stage in range(STAGES):
            for step in range(n_pts):
                unless_here(step, lambda: send(half, stage, step).wait_send())


def on_device(n_blk, n_pts, signal, offsets, kept, weights):
    seg, points = signal.shape
    blocks = offsets.shape[0]
    freq_all = kept.shape[0]
    freqs = freq_all // n_pts
    groups = n_pts // n_blk
    whole = n_blk * blocks
    halves = points // LANES
    part = blocks // STAGES
    hbm = pl.BlockSpec(memory_space=pltpu.HBM)
    return pl.pallas_call(
        functools.partial(kernel, n_blk, n_pts),
        out_shape=jax.ShapeDtypeStruct((freqs, 2, blocks, whole), jnp.float32),
        in_specs=[hbm, hbm, hbm, hbm],
        out_specs=pl.BlockSpec(memory_space=pltpu.VMEM),
        scratch_shapes=[
            [
                pltpu.VMEM(((seg + LANES) // ALIGN, ALIGN, LANES), jnp.bfloat16)
                for _ in range(halves)
            ],
            pltpu.VMEM((ALIGN, 2 * freq_all, SPAN), jnp.bfloat16),
            pltpu.VMEM((halves, STAGES, 2 * freq_all * part, LANES), jnp.float32),
            pltpu.VMEM((halves, STAGES, 2, freq_all, part, LANES), jnp.bfloat16),
            pltpu.VMEM((halves, groups, 2, freqs, n_blk, blocks, LANES), jnp.bfloat16),
            pltpu.VMEM((freqs, 2 * whole, 2 * whole), jnp.float32),
            pltpu.VMEM((n_blk, freqs, 2, blocks, whole), jnp.float32),
            pltpu.VMEM((n_blk, freqs, 2, blocks, whole), jnp.bfloat16),
            pltpu.VMEM((n_blk - 1, freqs, 2, blocks, whole), jnp.bfloat16),
            pltpu.SMEM(offsets.shape, jnp.int32),
            pltpu.SMEM(kept.shape, jnp.int32),
            pltpu.VMEM((1, points), jnp.float32),
            pltpu.SemaphoreType.DMA((halves, PIECES)),
            pltpu.SemaphoreType.DMA((3,)),
            pltpu.SemaphoreType.DMA((halves, STAGES, n_pts)),
            pltpu.SemaphoreType.DMA((halves, STAGES, groups, n_blk)),
            pltpu.SemaphoreType.DMA((n_blk - 1,)),
            pltpu.SemaphoreType.DMA((n_blk - 1,)),
        ],
        compiler_params=pltpu.CompilerParams(
            collective_id=0, has_side_effects=True, vmem_limit_bytes=60000 * 1024
        ),
    )(
        signal.reshape(seg // ALIGN, ALIGN, points),
        offsets,
        kept,
        weights.reshape(1, points),
    )


def solution(mesh):
    placed = (P("blk", "pts"), P("blk"), P(), P("pts"))
    return jax.shard_map(
        functools.partial(on_device, mesh.shape["blk"], mesh.shape["pts"]),
        mesh=mesh,
        in_specs=placed,
        out_specs=P("pts", None, "blk", None),
        check_vma=False,
    )
```
